32 devices in a mesh: env: 4 (over z), cand: 8 (over y, x, core).
Axes of the slice: x: 2, y: 2, z: 4, core: 2. Of those that a mesh axis runs over, the one named last changes fastest.
Arguments:
- white: bfloat16 [3, 64, 64, 4096], P(None, 'env', 'cand'), may hold values from -5 to 5
- mean_init: float32 [64, 2560], P('env'), may hold values from -0.3 to 0.3
- std_init: float32 [64, 2560], P('env'), may hold values from 0.05 to 0.8
- init_state: float32 [64, 128], P('env'), may hold values from -3 to 3
- goal_state: float32 [64, 128], P('env'), may hold values from -3 to 3
- w_state: bfloat16 [128, 512], replicated, may hold values from -0.5 to 0.5
- w_action: bfloat16 [64, 512], replicated, may hold values from -1.5 to 1.5
- w_out: bfloat16 [512, 128], replicated, may hold values from -0.25 to 0.25
- bias_in: float32 [512], replicated, may hold values from -3 to 3
- bias_out: float32 [128], replicated, may hold values from -3 to 3
- elite_idx: int32 [64, 3, 6], P('env'), may hold values from 0 to 63, all different within a row
Outputs:
- final_mean: float32 [64, 2560], P('env')
- final_std: float32 [64, 2560], P('env')
- costs: float32 [3, 64, 64], P(None, 'env', 'cand')
The draws below stay inside these ranges and needn't reach their ends.
Inputs may be any that keep to these rules, and one draw needn't show every extreme that they name: `elite_idx`: each row names 6 different candidates.
All inputs are finite; a program needn't handle non-finite values.
Results may differ from the reference program's by a relative error of at most 0.0031.
Values sent between devices are 32-bit elements; how exact they have to be, the bound alone decides.
A program may use at most 128 MiB of HBM per device.

```python
import math
import jax
import jax.numpy as jnp
from jax import lax

ENV_DEV = 16
ITERS = 3
HORIZON = 40
NOISE_LEN = 64
ACT = 64
STATE = 128
HIDDEN_SIZE = 512
ENVS = 64
CAND = 64
ELITES = 6


def steps_of(rng, shape, cuts, least, largest):
    factor_of, own = 1.0, jax.random.fold_in(rng, 6)
    for dim, shards_of in cuts:
        steps = jnp.exp(jax.random.uniform(jax.random.fold_in(own, dim), (shards_of,), jnp.float32, least / len(cuts), largest / len(cuts)))
        factor_of = factor_of * jnp.repeat(steps, shape[dim] // shards_of).reshape([-1 if axis == dim else 1 for axis in range(len(shape))])
    return factor_of


def choose_distinct(own_key, rows, number_of, top, lift):
    ranking = jax.random.permutation(jax.random.fold_in(own_key, 1), number_of)
    boost = ranking
    for power in range(3):
        boost = boost * boost // number_of
    boost = boost * lift // number_of
    tickets = jax.random.randint(jax.random.fold_in(own_key, 2), (rows, number_of), 0, 4096) + boost
    sure = jax.random.permutation(jax.random.fold_in(own_key, 3), rows)[jnp.arange(number_of) % rows]
    tickets = jnp.where(jnp.arange(rows)[:, None] == sure[None, :], 1 << 14, tickets)
    merit = tickets * number_of + jnp.arange(number_of)
    return lax.top_k(merit.astype(jnp.int32), top)[1].astype(jnp.int32)


def bell_draw(stream_key, dims, deviation, most, cuts=(), kind=jnp.bfloat16):
    array = deviation * jax.random.normal(stream_key, dims, jnp.float32)
    if cuts:
        array = array * steps_of(stream_key, dims, cuts, -0.22, 0.18)
    return jnp.clip(array, -most, most).astype(kind)


def setup_inputs(seed: int = 0) -> dict:
    keys = jax.random.split(jax.random.key(seed), 12)
    white = bell_draw(keys[0], (ITERS, ENVS, CAND, NOISE_LEN * ACT), 1.0, 5.0, ((1, 4), (2, 8)))
    mean_init = jnp.clip(jax.random.uniform(keys[1], (ENVS, HORIZON * ACT), jnp.float32, -0.3, 0.3) * steps_of(keys[1], (ENVS, HORIZON * ACT), ((0, 4),), -0.4, 0.0), -0.3, 0.3)
    std_init = jnp.clip(jnp.exp(math.log(0.8) - 2.7725887 * jax.random.uniform(keys[2], (ENVS, HORIZON * ACT), jnp.float32) ** steps_of(keys[2], (ENVS, HORIZON * ACT), ((0, 4),), -0.2, 0.2)), 0.05, 0.8)
    init_state = bell_draw(keys[3], (ENVS, STATE), 0.5, 3.0, ((0, 4),), jnp.float32)
    goal_state = bell_draw(keys[4], (ENVS, STATE), 0.5, 3.0, ((0, 4),), jnp.float32)
    w_state = bell_draw(keys[5], (STATE, HIDDEN_SIZE), STATE ** -0.5, 0.5)
    w_action = bell_draw(keys[6], (ACT, HIDDEN_SIZE), (ACT // 4) ** -0.5, 1.5)
    w_out = bell_draw(keys[7], (HIDDEN_SIZE, STATE), HIDDEN_SIZE ** -0.5, 0.25)
    bias_in = bell_draw(keys[8], (HIDDEN_SIZE,), 0.5, 3.0, (), jnp.float32)
    bias_out = bell_draw(keys[9], (STATE,), 0.5, 3.0, (), jnp.float32)
    elite_idx = choose_distinct(keys[10], ENVS * ITERS, CAND, ELITES, 0).reshape((ENVS, ITERS, ELITES))
    return dict(white=white, mean_init=mean_init, std_init=std_init, init_state=init_state, goal_state=goal_state, w_state=w_state, w_action=w_action, w_out=w_out, bias_in=bias_in, bias_out=bias_out, elite_idx=elite_idx)


BETA_EXP = 2.5
MOMENTUM = 0.1
FLOOR_SHARE = 0.1
ACT_COST = 0.1

def colored_ref(white_block):
    env_count, cand_count, flat = white_block.shape
    series = white_block.astype(jnp.float32).reshape(env_count, cand_count, NOISE_LEN, ACT)
    freqs = jnp.arange(NOISE_LEN // 2 + 1, dtype=jnp.int32)
    scale = (jnp.maximum(freqs, 1).astype(jnp.float32) / NOISE_LEN) ** (-BETA_EXP / 2)
    kernel = jnp.fft.irfft(scale, n=NOISE_LEN)
    kernel = kernel / jnp.sqrt(jnp.sum(kernel * kernel))
    kernel_low = lax.optimization_barrier(kernel.astype(jnp.bfloat16))
    kernel_back = kernel_low.astype(jnp.float32)
    kernel_freq = jnp.fft.rfft(kernel_back, n=NOISE_LEN)
    spectrum = jnp.fft.rfft(series, axis=2) * kernel_freq[None, None, :, None]
    colored = jnp.fft.irfft(spectrum, n=NOISE_LEN, axis=2)[:, :, :HORIZON, :]
    return colored.reshape(env_count, cand_count, HORIZON * ACT).astype(jnp.float32)

def rollout(actions, start, goal, w_state, w_action, w_out, bias_in, bias_out):
    ordered = jnp.swapaxes(actions, 0, 1)

    def advance(state, action):
        pre = jnp.dot(state.astype(jnp.bfloat16), w_state, preferred_element_type=jnp.float32)
        pre = pre + jnp.dot(action.astype(jnp.bfloat16), w_action, preferred_element_type=jnp.float32) + bias_in
        hidden = jax.nn.silu(pre).astype(jnp.bfloat16)
        state = jnp.tanh(state + jnp.dot(hidden, w_out, preferred_element_type=jnp.float32) + bias_out)
        error = state - goal
        step_cost = lax.optimization_barrier(jnp.mean(error * error, axis=-1)) + ACT_COST * lax.optimization_barrier(jnp.mean(action * action, axis=-1))
        return (state, step_cost)
    final, step_costs = lax.scan(advance, start, ordered)
    return lax.optimization_barrier(jnp.mean(step_costs, axis=0))

def reference(white, mean_init, std_init, init_state, goal_state, w_state, w_action, w_out, bias_in, bias_out, elite_idx):
    blocks = ENVS // ENV_DEV
    center, spread = (mean_init, std_init)
    cost_list = []
    for iteration in range(ITERS):

        def block_work(pieces):
            white_block, center_block, spread_block, start_block, goal_block, elite_block = pieces
            noise = colored_ref(white_block)
            actions = jnp.clip(center_block[:, None, :] + spread_block[:, None, :] * noise, -1.0, 1.0)
            rows = ENV_DEV * CAND
            starts = jnp.broadcast_to(start_block[:, None, :], (ENV_DEV, CAND, STATE)).reshape(rows, STATE)
            goals = jnp.broadcast_to(goal_block[:, None, :], (ENV_DEV, CAND, STATE)).reshape(rows, STATE)
            block_costs = rollout(actions.reshape(rows, HORIZON, ACT), starts, goals, w_state, w_action, w_out, bias_in, bias_out)
            member = lax.optimization_barrier(jnp.sum((elite_block[:, :, None] == jnp.arange(CAND, dtype=jnp.int32)[None, None, :]).astype(jnp.float32), axis=1))
            sums = jnp.einsum('ec,ech->eh', member, actions, precision=lax.Precision.HIGHEST)
            squares = jnp.einsum('ec,ech->eh', member, actions * actions, precision=lax.Precision.HIGHEST)
            return (block_costs.reshape(ENV_DEV, CAND), sums, squares)
        pieces = (white[iteration].reshape(blocks, ENV_DEV, CAND, NOISE_LEN * ACT), center.reshape(blocks, ENV_DEV, HORIZON * ACT), spread.reshape(blocks, ENV_DEV, HORIZON * ACT), init_state.reshape(blocks, ENV_DEV, STATE), goal_state.reshape(blocks, ENV_DEV, STATE), elite_idx[:, iteration, :].reshape(blocks, ENV_DEV, ELITES))
        block_costs, sums, squares = lax.map(block_work, pieces)
        cost_list.append(block_costs.reshape(ENVS, CAND))
        sums = sums.reshape(ENVS, HORIZON * ACT)
        squares = squares.reshape(ENVS, HORIZON * ACT)
        elite_mean = sums / ELITES
        variance = jnp.maximum(squares / ELITES - elite_mean * elite_mean, 0.0)
        center = MOMENTUM * center + (1.0 - MOMENTUM) * elite_mean
        mixed = MOMENTUM * spread + (1.0 - MOMENTUM) * jnp.sqrt(variance)
        env_peak = lax.optimization_barrier(jnp.max(mixed, axis=1))
        peak = jnp.max(env_peak)
        settled = jnp.mean(env_peak / peak)
        spread = jnp.maximum(mixed, FLOOR_SHARE * peak) * (0.5 + settled)
    return (center, spread, jnp.stack(cost_list))
```

```python
import functools

import jax
import jax.numpy as jnp
import numpy as np
from jax import lax
from jax.experimental import pallas as pl
from jax.experimental.pallas import tpu as pltpu
from jax.sharding import PartitionSpec as P

BETA_EXP = 2.5
MOMENTUM = 0.1
FLOOR_SHARE = 0.1
ACT_COST = 0.1
MESH = pl.DeviceIdType.MESH
LANES = 128
WIDE = 256
SUB = 8

WHILE_SUMS = ((), ((((0, 9), (1, 0)), 9),), ((((2, 0), (1, 16)), 4), (((2, 4),), 8)))
WHILE_PEAKS = ((((((0, 0),), 9)),), ((((0, 18), (1, 9)), 2), (((1, 11),), 5)), ((((2, 12),), 8),))


def color_rows(length, act):
    freqs = np.arange(length // 2 + 1)
    scale = (np.maximum(freqs, 1) / length) ** (-BETA_EXP / 2)
    kernel = np.fft.irfft(scale, n=length)
    kernel = kernel / np.sqrt(np.sum(kernel * kernel))
    q = WIDE // act
    row = np.arange(length)
    lane_step = np.arange(WIDE) // act
    shift = (q * (row // q))[:, None] + lane_step[None, :] - (row % q)[:, None]
    return jnp.asarray(kernel[shift % length], dtype=jnp.bfloat16).astype(jnp.float32)


def plan_kernel(
    dims,
    white_hbm,
    mean_hbm,
    std_hbm,
    start_hbm,
    goal_hbm,
    ws_hbm,
    wa_hbm,
    wo_hbm,
    bi_hbm,
    bo_hbm,
    elite_hbm,
    color_hbm,
    fmean_ref,
    fstd_ref,
    cost_out,
    white,
    mean_ref,
    std_ref,
    start_ref,
    goal_ref,
    ws_ref,
    wa_ref,
    wo_ref,
    bi_ref,
    bo_ref,
    elite_ref,
    color_ref,
    table,
    noise,
    acts,
    w_pair,
    state,
    goals,
    cost,
    member,
    cen,
    spr,
    part,
    rs_recv,
    ag,
    z_send,
    z_recv,
    copy_sem,
    send_sem,
    recv_sem,
):
    iters, env_dev, cand_dev, act, tiles, units, share, n_cand, n_env, elites = dims
    rows = env_dev * cand_dev
    state_dim = start_ref.shape[1]
    halves = env_dev // SUB
    n_units = tiles * halves
    n_all = n_cand * n_env
    length_blocks = white.shape[1] // WIDE
    out_blocks = tiles * LANES // WIDE
    low_block = length_blocks - out_blocks + 1
    per_tile = LANES // act
    me = lax.axis_index("cand")
    me_env = lax.axis_index("env")

    pairs = (
        (color_hbm, color_ref),
        (white_hbm.at[pl.ds(0, rows)], white.at[pl.ds(0, rows)]),
        (elite_hbm, elite_ref),
        (mean_hbm, mean_ref),
        (std_hbm, std_ref),
        (start_hbm, start_ref),
        (goal_hbm, goal_ref),
        (ws_hbm, ws_ref),
        (wa_hbm, wa_ref),
        (wo_hbm, wo_ref),
        (bi_hbm, bi_ref),
        (bo_hbm, bo_ref),
        (
            white_hbm.at[pl.ds(rows, (iters - 1) * rows)],
            white.at[pl.ds(rows, (iters - 1) * rows)],
        ),
    )
    loads = [
        pltpu.make_async_copy(src, dst, copy_sem.at[at]) for at, (src, dst) in enumerate(pairs)
    ]
    for load in loads:
        load.start()

    def peer_of(k):
        return {
            "env": lax.rem(me_env + k // n_cand, n_env),
            "cand": lax.rem(me + k % n_cand, n_cand),
        }

    def every_peer(visit):
        if n_all <= 64:
            for k in range(1, n_all):
                visit(k)
        else:
            lax.fori_loop(1, n_all, lambda k, carry: (visit(k), carry)[1], 0)

    barrier = pltpu.get_barrier_semaphore()
    every_peer(
        lambda k: pl.semaphore_signal(barrier, inc=1, device_id=peer_of(k), device_id_type=MESH)
    )

    q = WIDE // act
    eye = (
        lax.broadcasted_iota(jnp.int32, (act, WIDE), 0)
        == lax.broadcasted_iota(jnp.int32, (act, WIDE), 1) % act
    )

    def build(block, carry):
        shift = lax.rem(2 * length_blocks - (block + low_block), length_blocks)
        for j in range(q):
            line = color_ref[shift, j : j + 1, :]
            piece = jnp.where(eye, line, 0.0).astype(jnp.bfloat16)
            table[pl.ds(pl.multiple_of(block * WIDE + j * act, act), act), :] = piece
        return carry

    loads[0].wait()
    lax.fori_loop(0, table.shape[0] // WIDE, build, 0)

    for load in loads[2:-1]:
        load.wait()
    w_pair[...] = jnp.zeros_like(w_pair)
    for p in range(per_tile):
        w_pair[p, :state_dim, :] = ws_ref[...] * jnp.bfloat16(0.5)
        w_pair[p, state_dim + p * act : state_dim + (p + 1) * act, :] = wa_ref[...] * jnp.bfloat16(0.5)
    diagonal = lax.broadcasted_iota(jnp.int32, (env_dev, env_dev), 0) == lax.broadcasted_iota(
        jnp.int32, (env_dev, env_dev), 1
    )
    for it in range(iters):
        own = elite_ref[it]
        for c in range(cand_dev):
            hit = (own == me * cand_dev + c).astype(jnp.float32)
            hit = jnp.sum(hit, axis=0, keepdims=True)
            hit = jnp.sum(jnp.where(diagonal, hit, 0.0), axis=1, keepdims=True)
            member[it, c] = jnp.broadcast_to(hit, (env_dev, LANES))
    for c in range(cand_dev):
        spot = slice(c * env_dev, (c + 1) * env_dev)
        goals[spot, :] = goal_ref[...]
        for it in range(iters):
            state[it, spot, :] = start_ref[...]
    cost[...] = jnp.zeros_like(cost)
    if units > n_units:
        cen[...] = jnp.zeros_like(cen)
        spr[...] = jnp.zeros_like(spr)
        part[...] = jnp.zeros_like(part)
    for tile in range(tiles):
        for h in range(halves):
            at = (slice(h * SUB, (h + 1) * SUB), slice(tile * LANES, (tile + 1) * LANES))
            cen[tile * halves + h] = mean_ref[at]
            spr[tile * halves + h] = std_ref[at]

    def color(first, size):
        spot = slice(first, first + size)
        group = 2 if out_blocks % 2 == 0 else 1

        def one(step, carry):
            for g in range(group):
                block = step * group + g
                start = pl.multiple_of((out_blocks - 1 - block) * WIDE, WIDE)
                band = table[pl.ds(start, white.shape[1]), :]
                out = jnp.dot(white[spot, :], band, preferred_element_type=jnp.float32)
                for p in range(WIDE // LANES):
                    noise[block * (WIDE // LANES) + p, spot, :] = out[:, p * LANES : (p + 1) * LANES]
            return carry

        lax.fori_loop(0, out_blocks // group, one, 0)

    act_weight = ACT_COST * state_dim / act

    def model(it, unit, scales):
        if it == 0:
            return cen[unit], spr[unit]
        floor, gain = scales
        return ag[it - 1, unit, 0], jnp.maximum(ag[it - 1, unit, 1], floor) * gain

    def make_actions(it, scales):
        def one(tile, carry):
            fitted = [model(it, tile * halves + h, scales) for h in range(halves)]
            center = jnp.concatenate([f[0] for f in fitted], axis=0)
            spread = jnp.concatenate([f[1] for f in fitted], axis=0)
            sums = jnp.zeros((env_dev, LANES), jnp.float32)
            squares = jnp.zeros((env_dev, LANES), jnp.float32)
            for c in range(cand_dev):
                drawn = noise[tile, pl.ds(it * rows + c, env_dev, stride=cand_dev), :]
                action = jnp.clip(center + spread * drawn, -1.0, 1.0)
                spot = slice(c * env_dev, (c + 1) * env_dev)
                acts[it, tile, spot, :] = action.astype(jnp.bfloat16)
                chosen = member[it, c] * action
                square = action * action
                sums = sums + chosen
                squares = squares + chosen * action
                cost[it, spot, :] += act_weight * square
            sums = sums.reshape(halves, SUB, LANES)
            squares = squares.reshape(halves, SUB, LANES)
            for h in range(halves):
                part[it, tile * halves + h, 0] = sums[h]
                part[it, tile * halves + h, 1] = squares[h]
            return carry

        lax.fori_loop(0, tiles, one, 0)

    def scatter_copies(it):
        for o in range(1, n_cand):
            peer = lax.rem(me + o, n_cand)
            yield pltpu.make_async_remote_copy(
                src_ref=part.at[it, pl.ds(peer * share, share)],
                dst_ref=rs_recv.at[it, o - 1],
                send_sem=send_sem.at[it, 0],
                recv_sem=recv_sem.at[it, 0],
                device_id={"cand": peer},
                device_id_type=MESH,
            )

    def gather_copies(it):
        mine = ag.at[it, pl.ds(me * share, share)]
        for o in range(1, n_cand):
            yield pltpu.make_async_remote_copy(
                src_ref=mine,
                dst_ref=mine,
                send_sem=send_sem.at[it, 1],
                recv_sem=recv_sem.at[it, 1],
                device_id={"cand": lax.rem(me + o, n_cand)},
                device_id_type=MESH,
            )

    def send_peaks(it):
        every_peer(
            lambda k: pltpu.make_async_remote_copy(
                src_ref=z_send.at[it],
                dst_ref=z_recv.at[it, k],
                send_sem=send_sem.at[it, 2],
                recv_sem=recv_sem.at[it, 2],
                device_id=peer_of(k),
                device_id_type=MESH,
            ).start()
        )

    def await_bytes(stage, it, sem):
        others = (n_cand - 1) * share
        ref = (rs_recv.at[it], ag.at[it, pl.ds(0, others)], z_recv.at[it, pl.ds(1, n_all - 1)])[stage]
        pltpu.make_async_copy(ref, ref, sem.at[it, stage]).wait()

    def send_sums(it):
        for copy in scatter_copies(it):
            copy.start()

    def refit(it, scales):
        await_bytes(0, it, recv_sem)
        mine = pl.ds(me * share, share)
        total = part[it, mine] + jnp.sum(rs_recv[it], axis=0)
        mean = total[:, 0] / elites
        deviation = jnp.sqrt(jnp.maximum(total[:, 1] / elites - mean * mean, 0.0))
        center, spread = model(it, mine, scales)
        mixed = MOMENTUM * spread + (1.0 - MOMENTUM) * deviation
        lane = lax.broadcasted_iota(jnp.int32, (SUB, LANES), 1)
        sub = lax.broadcasted_iota(jnp.int32, (SUB, LANES), 0)
        row = jnp.zeros((SUB, LANES), jnp.float32)
        for i in range(share):
            half = lax.rem(me * share + i, halves)
            best = jnp.max(mixed[i], axis=1, keepdims=True)
            row = jnp.maximum(row, jnp.where(lane == half * SUB + sub, best, 0.0))
        row = jnp.max(row, axis=0, keepdims=True)
        z_send[it] = row
        z_recv[it, 0] = row
        send_peaks(it)
        ag[it, mine, 0] = MOMENTUM * center + (1.0 - MOMENTUM) * mean
        ag[it, mine, 1] = mixed
        for copy in gather_copies(it):
            copy.start()

    def settle(it):
        await_bytes(2, it, recv_sem)
        peaks = jnp.max(z_recv[it].reshape(n_env, n_cand, 1, LANES), axis=1)
        peak = jnp.max(jnp.max(peaks, axis=0), axis=1, keepdims=True)
        settled = jnp.sum(jnp.sum(peaks, axis=0), axis=1, keepdims=True) / peak / (env_dev * n_env)
        floor = jnp.broadcast_to(FLOOR_SHARE * peak, (SUB, LANES))
        gain = jnp.broadcast_to(0.5 + settled, (SUB, LANES))
        await_bytes(1, it, recv_sem)
        return floor, gain

    def rollout(chains, count):
        bias_h = bi_ref[...] * 0.5
        bias_o = bo_ref[...]
        its = [it for it, _ in chains]

        def steps(i, carry):
            for p in range(per_tile):
                hidden = []
                for it, low in chains:
                    x = jnp.concatenate([state[it].astype(jnp.bfloat16), acts[it, low + i]], axis=1)
                    h = jnp.dot(x, w_pair[p], preferred_element_type=jnp.float32) + bias_h
                    hidden.append((h * jnp.tanh(h) + h).astype(jnp.bfloat16))
                for it, hid in zip(its, hidden):
                    delta = jnp.dot(hid, wo_ref[...], preferred_element_type=jnp.float32)
                    then = jnp.tanh(state[it] + delta + bias_o)
                    error = then - goals[...]
                    cost[it] += error * error
                    state[it] = then
            return carry

        lax.fori_loop(0, count, steps, 0)

    def work(groups):
        for chains, count in groups:
            rollout(
                tuple((it, low * tiles // 20) for it, low in chains), count * tiles // 20
            )

    loads[1].wait()
    color(0, rows)
    scales = None
    for it in range(iters):
        make_actions(it, scales)
        if it == 0:
            pl.semaphore_wait(barrier, n_all - 1)
        send_sums(it)
        if it == 0:
            loads[-1].wait()
            color(rows, (iters - 1) * rows)
        work(WHILE_SUMS[it])
        refit(it, scales)
        work(WHILE_PEAKS[it])
        scales = settle(it)

    for tile in range(tiles):
        for h in range(halves):
            at = (slice(h * SUB, (h + 1) * SUB), slice(tile * LANES, (tile + 1) * LANES))
            fmean_ref[at], fstd_ref[at] = model(iters, tile * halves + h, scales)
    scale = 1.0 / (state_dim * tiles * per_tile)
    for it in range(iters):
        for c in range(cand_dev):
            total = jnp.sum(cost[it, c * env_dev : (c + 1) * env_dev, :], axis=1, keepdims=True)
            line = jnp.sum(jnp.where(diagonal, total * scale, 0.0), axis=0, keepdims=True)
            cost_out[it, c : c + 1, :] = line
    for it in range(iters):
        for stage in range(3):
            await_bytes(stage, it, send_sem)


def shards(
    white,
    mean_init,
    std_init,
    init_state,
    goal_state,
    w_state,
    w_action,
    w_out,
    bias_in,
    bias_out,
    elite_idx,
):
    iters, env_dev, cand_dev, flat = white.shape
    act, hidden = w_action.shape
    state_dim = w_state.shape[0]
    hor_act = mean_init.shape[1]
    n_cand = lax.axis_size("cand")
    n_env = lax.axis_size("env")
    tiles = hor_act // LANES
    halves = env_dev // SUB
    share = -(-tiles * halves // n_cand)
    units = share * n_cand
    rows = env_dev * cand_dev
    out_blocks = hor_act // WIDE
    table_rows = flat + (out_blocks - 1) * WIDE
    dims = (iters, env_dev, cand_dev, act, tiles, units, share, n_cand, n_env, elite_idx.shape[2])
    hbm = pl.BlockSpec(memory_space=pl.ANY)
    vmem = pl.BlockSpec(memory_space=pltpu.VMEM)
    f32, bf16 = jnp.float32, jnp.bfloat16
    outs = (
        ((env_dev, hor_act), f32),
        ((env_dev, hor_act), f32),
        ((iters, cand_dev, env_dev), f32),
    )
    operands = (
        white.reshape(iters * rows, flat),
        mean_init,
        std_init,
        init_state,
        goal_state,
        w_state,
        w_action,
        w_out,
        bias_in.reshape(1, hidden),
        bias_out.reshape(1, state_dim),
        jnp.transpose(elite_idx, (1, 2, 0)),
        color_rows(flat // act, act).reshape(-1, WIDE // act, WIDE),
    )
    fmean, fstd, cost = pl.pallas_call(
        functools.partial(plan_kernel, dims),
        out_shape=tuple(pltpu.VMEM(shape, kind) for shape, kind in outs),
        in_specs=[hbm] * len(operands),
        out_specs=(vmem, vmem, vmem),
        scratch_shapes=[
            *(pltpu.VMEM(operand.shape, operand.dtype) for operand in operands),
            pltpu.VMEM((table_rows, WIDE), bf16),
            pltpu.VMEM((tiles, iters * rows, LANES), f32),
            pltpu.VMEM((iters, tiles, rows, LANES), bf16),
            pltpu.VMEM((LANES // act, state_dim + LANES, hidden), bf16),
            pltpu.VMEM((iters, rows, state_dim), f32),
            pltpu.VMEM((rows, state_dim), f32),
            pltpu.VMEM((iters, rows, LANES), f32),
            pltpu.VMEM((iters, cand_dev, env_dev, LANES), f32),
            pltpu.VMEM((units, SUB, LANES), f32),
            pltpu.VMEM((units, SUB, LANES), f32),
            pltpu.VMEM((iters, units, 2, SUB, LANES), f32),
            pltpu.VMEM((iters, n_cand - 1, share, 2, SUB, LANES), f32),
            pltpu.VMEM((iters, units, 2, SUB, LANES), f32),
            pltpu.VMEM((iters, 1, LANES), f32),
            pltpu.VMEM((iters, n_cand * n_env, 1, LANES), f32),
            pltpu.SemaphoreType.DMA((len(operands) + 1,)),
            pltpu.SemaphoreType.DMA((iters, 3)),
            pltpu.SemaphoreType.DMA((iters, 3)),
        ],
        compiler_params=pltpu.CompilerParams(collective_id=0, has_side_effects=True),
    )(*operands)
    return fmean, fstd, jnp.swapaxes(cost, 1, 2)


def solution(mesh):
    in_specs = (
        P(None, "env", "cand", None),
        P("env", None),
        P("env", None),
        P("env", None),
        P("env", None),
        P(),
        P(),
        P(),
        P(),
        P(),
        P("env", None, None),
    )
    out_specs = (P("env", None), P("env", None), P(None, "env", "cand"))
    return jax.shard_map(shards, mesh=mesh, in_specs=in_specs, out_specs=out_specs, check_vma=False)
```

```python
import functools

import jax
import jax.numpy as jnp
import numpy as np
from jax import lax
from jax.experimental import pallas as pl
from jax.experimental.pallas import tpu as pltpu
from jax.sharding import PartitionSpec as P

BETA_EXP = 2.5
MOMENTUM = 0.1
FLOOR_SHARE = 0.1
ACT_COST = 0.1
MESH = pl.DeviceIdType.MESH
LANES = 128
WIDE = 256
SUB = 8

TRIPS = 10
WHILE_EARLY = (
    ((((0, 0),), 2, 1, (1, 0)),),
    ((((0, 6), (1, 0)), 2, 1, (2, 0)),),
    ((((2, 0), (1, 6)), 2, 2, None),),
)
WHILE_LATE = ((), (), ())
WHILE_PEAKS = (
    ((((0, 2),), 3, 1, (1, 4)), (((0, 5),), 1, 1, None)),
    ((((0, 8), (1, 2)), 2, 1, (2, 4)), (((1, 4),), 1, 1, (2, 8)), (((1, 5),), 1, 1, None)),
    ((((2, 4),), 3, 2, None),),
)


def color_rows(length, act):
    freqs = np.arange(length // 2 + 1)
    scale = (np.maximum(freqs, 1) / length) ** (-BETA_EXP / 2)
    kernel = np.fft.irfft(scale, n=length)
    kernel = kernel / np.sqrt(np.sum(kernel * kernel))
    q = WIDE // act
    row = np.arange(length)
    lane_step = np.arange(WIDE) // act
    shift = (q * (row // q))[:, None] + lane_step[None, :] - (row % q)[:, None]
    return jnp.asarray(kernel[shift % length], dtype=jnp.bfloat16).astype(jnp.float32)


def plan_kernel(
    dims,
    white_hbm,
    mean_hbm,
    std_hbm,
    start_hbm,
    goal_hbm,
    ws_hbm,
    wa_hbm,
    wo_hbm,
    bi_hbm,
    bo_hbm,
    elite_hbm,
    color_hbm,
    fmean_ref,
    fstd_ref,
    cost_out,
    white,
    mean_ref,
    std_ref,
    start_ref,
    goal_ref,
    ws_ref,
    wa_ref,
    wo_ref,
    bi_ref,
    bo_ref,
    elite_ref,
    color_ref,
    table,
    noise,
    acts,
    w_pair,
    state,
    goals,
    cost,
    member,
    cen,
    spr,
    part,
    rs_recv,
    ag,
    z_send,
    z_recv,
    copy_sem,
    send_sem,
    recv_sem,
):
    iters, env_dev, cand_dev, act, tiles, units, share, n_cand, n_env, elites = dims
    rows = env_dev * cand_dev
    state_dim = start_ref.shape[1]
    halves = env_dev // SUB
    n_units = tiles * halves
    n_all = n_cand * n_env
    length_blocks = white.shape[1] // WIDE
    out_blocks = tiles * LANES // WIDE
    low_block = length_blocks - out_blocks + 1
    per_tile = LANES // act
    me = lax.axis_index("cand")
    me_env = lax.axis_index("env")

    pairs = (
        (color_hbm, color_ref),
        (white_hbm.at[pl.ds(0, rows)], white.at[pl.ds(0, rows)]),
        (elite_hbm, elite_ref),
        (mean_hbm, mean_ref),
        (std_hbm, std_ref),
        (start_hbm, start_ref),
        (goal_hbm, goal_ref),
        (ws_hbm, ws_ref),
        (wa_hbm, wa_ref),
        (wo_hbm, wo_ref),
        (bi_hbm, bi_ref),
        (bo_hbm, bo_ref),
        (
            white_hbm.at[pl.ds(rows, (iters - 1) * rows)],
            white.at[pl.ds(rows, (iters - 1) * rows)],
        ),
    )
    loads = [
        pltpu.make_async_copy(src, dst, copy_sem.at[at]) for at, (src, dst) in enumerate(pairs)
    ]
    for load in loads[:-1]:
        load.start()

    def peer_of(k):
        return {
            "env": lax.rem(me_env + k // n_cand, n_env),
            "cand": lax.rem(me + k % n_cand, n_cand),
        }

    def every_peer(visit):
        if n_all <= 64:
            for k in range(1, n_all):
                visit(k)
        else:
            lax.fori_loop(1, n_all, lambda k, carry: (visit(k), carry)[1], 0)

    barrier = pltpu.get_barrier_semaphore()
    every_peer(
        lambda k: pl.semaphore_signal(barrier, inc=1, device_id=peer_of(k), device_id_type=MESH)
    )

    q = WIDE // act
    eye = (
        lax.broadcasted_iota(jnp.int32, (act, WIDE), 0)
        == lax.broadcasted_iota(jnp.int32, (act, WIDE), 1) % act
    )

    def build(places, block, carry):
        shift = lax.rem(2 * length_blocks - (block + low_block), length_blocks)
        for j in range(q):
            line = color_ref[shift, j : j + 1, :]
            piece = jnp.where(eye, line, 0.0).astype(jnp.bfloat16)
            for place in places:
                start = pl.multiple_of((block + place) * WIDE + j * act, act)
                table[pl.ds(start, act), :] = piece
        return carry

    diagonal = lax.broadcasted_iota(jnp.int32, (env_dev, env_dev), 0) == lax.broadcasted_iota(
        jnp.int32, (env_dev, env_dev), 1
    )

    def mark_elites(it):
        own = elite_ref[it]
        for c in range(cand_dev):
            hit = (own == me * cand_dev + c).astype(jnp.float32)
            hit = jnp.sum(hit, axis=0, keepdims=True)
            hit = jnp.sum(jnp.where(diagonal, hit, 0.0), axis=1, keepdims=True)
            member[it, c] = jnp.broadcast_to(hit, (env_dev, LANES))

    def set_first():
        for load in loads[2:5]:
            load.wait()
        mark_elites(0)
        cost[...] = jnp.zeros_like(cost)
        if units > n_units:
            cen[...] = jnp.zeros_like(cen)
            spr[...] = jnp.zeros_like(spr)
            part[...] = jnp.zeros_like(part)
        for tile in range(tiles):
            for h in range(halves):
                at = (slice(h * SUB, (h + 1) * SUB), slice(tile * LANES, (tile + 1) * LANES))
                cen[tile * halves + h] = mean_ref[at]
                spr[tile * halves + h] = std_ref[at]

    def set_rest():
        for load in loads[5:]:
            load.wait()
        w_pair[...] = jnp.zeros_like(w_pair)
        for p in range(per_tile):
            w_pair[p, :state_dim, :] = ws_ref[...] * jnp.bfloat16(0.5)
            w_pair[p, state_dim + p * act : state_dim + (p + 1) * act, :] = wa_ref[...] * jnp.bfloat16(0.5)
        for it in range(1, iters):
            mark_elites(it)
        for c in range(cand_dev):
            spot = slice(c * env_dev, (c + 1) * env_dev)
            goals[spot, :] = goal_ref[...]
            for it in range(iters):
                state[it, spot, :] = start_ref[...]

    n_blocks = table.shape[0] // WIDE
    twice = min(max(n_blocks - length_blocks, 0), length_blocks)
    loads[0].wait()
    lax.fori_loop(0, twice, functools.partial(build, (0, length_blocks)), 0)
    lax.fori_loop(twice, min(length_blocks, n_blocks), functools.partial(build, (0,)), 0)
    loads[-1].start()
    set_first()

    def color_block(it, block):
        spot = pl.ds(it * rows, rows)
        start = pl.multiple_of((out_blocks - 1 - block) * WIDE, WIDE)
        band = table[pl.ds(start, white.shape[1]), :]
        out = jnp.dot(white[spot, :], band, preferred_element_type=jnp.float32)
        for p in range(WIDE // LANES):
            noise[block * (WIDE // LANES) + p, spot, :] = out[:, p * LANES : (p + 1) * LANES]

    def color_piece(it, block, piece, pieces):
        spot = pl.ds(it * rows, rows)
        width = white.shape[1] // pieces
        start = pl.multiple_of((out_blocks - 1 - block) * WIDE + piece * width, WIDE)
        band = table[pl.ds(start, width), :]
        taken = white[spot, piece * width : (piece + 1) * width]
        out = jnp.dot(taken, band, preferred_element_type=jnp.float32)
        for p in range(WIDE // LANES):
            half = out[:, p * LANES : (p + 1) * LANES]
            at = block * (WIDE // LANES) + p
            noise[at, spot, :] = half if piece == 0 else noise[at, spot, :] + half

    def color(it, first, count, group):
        def one(step, carry):
            for g in range(group):
                color_block(it, first + step * group + g)
            return carry

        lax.fori_loop(0, count // group, one, 0)

    act_weight = ACT_COST * state_dim / act

    def model(it, unit, scales):
        if it == 0:
            return cen[unit], spr[unit]
        floor, gain = scales
        return ag[it - 1, unit, 0], jnp.maximum(ag[it - 1, unit, 1], floor) * gain

    def make_actions(it, scales, first, count):
        def one(tile, carry):
            fitted = [model(it, tile * halves + h, scales) for h in range(halves)]
            center = jnp.concatenate([f[0] for f in fitted], axis=0)
            spread = jnp.concatenate([f[1] for f in fitted], axis=0)
            sums = jnp.zeros((env_dev, LANES), jnp.float32)
            squares = jnp.zeros((env_dev, LANES), jnp.float32)
            for c in range(cand_dev):
                drawn = noise[tile, pl.ds(it * rows + c, env_dev, stride=cand_dev), :]
                action = jnp.clip(center + spread * drawn, -1.0, 1.0)
                spot = slice(c * env_dev, (c + 1) * env_dev)
                acts[it, tile, spot, :] = action.astype(jnp.bfloat16)
                chosen = member[it, c] * action
                square = action * action
                sums = sums + chosen
                squares = squares + chosen * action
                cost[it, spot, :] += act_weight * square
            sums = sums.reshape(halves, SUB, LANES)
            squares = squares.reshape(halves, SUB, LANES)
            for h in range(halves):
                part[it, tile * halves + h, 0] = sums[h]
                part[it, tile * halves + h, 1] = squares[h]
            return carry

        lax.fori_loop(first, first + count, one, 0)

    parts = 2 if units == n_units and n_cand % 2 == 0 and out_blocks % 2 == 0 else 1
    crowd = n_cand // parts
    near = me // crowd

    lots = ((0, share // 2), (share // 2, share - share // 2)) if share > 1 else ((0, share),)
    sums_stage, means_stage, peaks_stage = 0, len(lots), 2 * len(lots)

    def send_sums(it, part_at, far, lot):
        low, size = lots[lot]
        for o in range(0 if far else 1, crowd):
            peer = part_at * crowd + lax.rem(lax.rem(me, crowd) + o, crowd)
            pltpu.make_async_remote_copy(
                src_ref=part.at[it, pl.ds(peer * share + low, size)],
                dst_ref=rs_recv.at[it, o if far else n_cand - crowd + o - 1, pl.ds(low, size)],
                send_sem=send_sem.at[it, sums_stage + lot],
                recv_sem=recv_sem.at[it, sums_stage + lot],
                device_id={"cand": peer},
                device_id_type=MESH,
            ).start()

    def send_means(it, lot):
        low, size = lots[lot]
        mine = ag.at[it, pl.ds(me * share + low, size)]
        for o in range(1, n_cand):
            pltpu.make_async_remote_copy(
                src_ref=mine,
                dst_ref=mine,
                send_sem=send_sem.at[it, means_stage + lot],
                recv_sem=recv_sem.at[it, means_stage + lot],
                device_id={"cand": lax.rem(me + o, n_cand)},
                device_id_type=MESH,
            ).start()

    def send_peaks(it):
        every_peer(
            lambda k: pltpu.make_async_remote_copy(
                src_ref=z_send.at[it],
                dst_ref=z_recv.at[it, k],
                send_sem=send_sem.at[it, peaks_stage],
                recv_sem=recv_sem.at[it, peaks_stage],
                device_id=peer_of(k),
                device_id_type=MESH,
            ).start()
        )

    def await_bytes(stage, it, sem):
        if stage == peaks_stage:
            ref = z_recv.at[it, pl.ds(1, n_all - 1)]
        elif stage < means_stage:
            low, size = lots[stage]
            ref = rs_recv.at[it, pl.ds(0, n_cand - 1), pl.ds(low, size)]
        else:
            ref = ag.at[it, pl.ds(0, (n_cand - 1) * lots[stage - means_stage][1])]
        pltpu.make_async_copy(ref, ref, sem.at[it, stage]).wait()

    def refit(it, scales, lot):
        low, size = lots[lot]
        await_bytes(sums_stage + lot, it, recv_sem)
        mine = pl.ds(me * share + low, size)
        total = part[it, mine] + jnp.sum(rs_recv[it, :, low : low + size], axis=0)
        mean = total[:, 0] / elites
        deviation = jnp.sqrt(jnp.maximum(total[:, 1] / elites - mean * mean, 0.0))
        center, spread = model(it, mine, scales)
        mixed = MOMENTUM * spread + (1.0 - MOMENTUM) * deviation
        ag[it, mine, 0] = MOMENTUM * center + (1.0 - MOMENTUM) * mean
        ag[it, mine, 1] = mixed
        lane = lax.broadcasted_iota(jnp.int32, (SUB, LANES), 1)
        sub = lax.broadcasted_iota(jnp.int32, (SUB, LANES), 0)
        row = jnp.zeros((SUB, LANES), jnp.float32)
        for i in range(size):
            half = lax.rem(me * share + low + i, halves)
            best = jnp.max(mixed[i], axis=1, keepdims=True)
            row = jnp.maximum(row, jnp.where(lane == half * SUB + sub, best, 0.0))
        row = jnp.max(row, axis=0, keepdims=True)
        if lot:
            row = jnp.maximum(row, z_send[it])
        z_send[it] = row
        if lot == len(lots) - 1:
            z_recv[it, 0] = row
            send_peaks(it)
        send_means(it, lot)

    def settle(it):
        await_bytes(peaks_stage, it, recv_sem)
        peaks = jnp.max(z_recv[it].reshape(n_env, n_cand, 1, LANES), axis=1)
        peak = jnp.max(jnp.max(peaks, axis=0), axis=1, keepdims=True)
        settled = jnp.sum(jnp.sum(peaks, axis=0), axis=1, keepdims=True) / peak / (env_dev * n_env)
        floor = jnp.broadcast_to(FLOOR_SHARE * peak, (SUB, LANES))
        gain = jnp.broadcast_to(0.5 + settled, (SUB, LANES))
        for lot in range(len(lots)):
            await_bytes(means_stage + lot, it, recv_sem)
        return floor, gain

    per_trip = -(-tiles // TRIPS)

    def rollout(chains, count, span, paint):
        bias_h = bi_ref[...] * 0.5
        bias_o = bo_ref[...]
        its = [it for it, _ in chains]

        def steps(i, carry):
            pieces = span * per_trip * per_tile
            for s in range(pieces):
                tile, p = s // per_tile, s % per_tile
                hidden = []
                for it, low in chains:
                    action = acts[it, (low + i * span) * per_trip + tile]
                    x = jnp.concatenate([state[it].astype(jnp.bfloat16), action], axis=1)
                    h = jnp.dot(x, w_pair[p], preferred_element_type=jnp.float32) + bias_h
                    hidden.append((h * jnp.tanh(h) + h).astype(jnp.bfloat16))
                if paint is not None:
                    color_piece(paint[0], paint[1] + i * 2, s, pieces)
                for it, hid in zip(its, hidden):
                    delta = jnp.dot(hid, wo_ref[...], preferred_element_type=jnp.float32)
                    then = jnp.tanh((state[it] + bias_o) + delta)
                    error = then - goals[...]
                    cost[it] += error * error
                    state[it] = then
                if paint is not None:
                    color_piece(paint[0], paint[1] + i * 2 + 1, s, pieces)
            return carry

        lax.fori_loop(0, count, steps, 0)

    def work(groups):
        for chains, count, span, paint in groups:
            rollout(chains, count, span, paint)

    loads[1].wait()
    scales = None
    half = out_blocks // parts
    everything = range(len(lots))
    for it in range(iters):
        for k in range(parts):
            far = k < parts - 1
            at = lax.rem(near + 1 + k, parts)
            if it == 0:
                color(0, at * half, half, half)
            make_actions(it, scales, at * (tiles // parts), tiles // parts)
            if it == 0 and k == 0:
                pl.semaphore_wait(barrier, n_all - 1)
            for lot in everything if it == 0 or parts == 1 else (0,):
                send_sums(it, at, far, lot)
        if it and parts > 1:
            for k in range(parts):
                for lot in everything[1:]:
                    send_sums(it, lax.rem(near + 1 + k, parts), k < parts - 1, lot)
        if it == 0:
            set_rest()
        work(WHILE_EARLY[it])
        if len(lots) > 1:
            refit(it, scales, 0)
        work(WHILE_LATE[it])
        refit(it, scales, len(lots) - 1)
        work(WHILE_PEAKS[it])
        if it == iters - 1:
            scale = 1.0 / (state_dim * tiles * per_tile)
            for i in range(iters):
                for c in range(cand_dev):
                    total = jnp.sum(cost[i, c * env_dev : (c + 1) * env_dev, :], axis=1, keepdims=True)
                    line = jnp.sum(jnp.where(diagonal, total * scale, 0.0), axis=0, keepdims=True)
                    cost_out[i, c : c + 1, :] = line
        scales = settle(it)

    for tile in range(tiles):
        for h in range(halves):
            at = (slice(h * SUB, (h + 1) * SUB), slice(tile * LANES, (tile + 1) * LANES))
            fmean_ref[at], fstd_ref[at] = model(iters, tile * halves + h, scales)
    for it in range(iters):
        for stage in range(peaks_stage + 1):
            await_bytes(stage, it, send_sem)


def store_kernel(fmean_ref, fstd_ref, cost_ref, fmean_hbm, fstd_hbm, cost_hbm, sem):
    copies = [
        pltpu.make_async_copy(src, dst, sem.at[at])
        for at, (src, dst) in enumerate(
            ((fmean_ref, fmean_hbm), (fstd_ref, fstd_hbm), (cost_ref, cost_hbm))
        )
    ]
    for copy in copies:
        copy.start()
    for copy in copies:
        copy.wait()


def shards(
    white,
    mean_init,
    std_init,
    init_state,
    goal_state,
    w_state,
    w_action,
    w_out,
    bias_in,
    bias_out,
    elite_idx,
):
    iters, env_dev, cand_dev, flat = white.shape
    act, hidden = w_action.shape
    state_dim = w_state.shape[0]
    hor_act = mean_init.shape[1]
    n_cand = lax.axis_size("cand")
    n_env = lax.axis_size("env")
    tiles = hor_act // LANES
    halves = env_dev // SUB
    share = -(-tiles * halves // n_cand)
    units = share * n_cand
    rows = env_dev * cand_dev
    out_blocks = hor_act // WIDE
    table_rows = flat + (out_blocks - 1) * WIDE
    dims = (iters, env_dev, cand_dev, act, tiles, units, share, n_cand, n_env, elite_idx.shape[2])
    hbm = pl.BlockSpec(memory_space=pl.ANY)
    vmem = pl.BlockSpec(memory_space=pltpu.VMEM)
    f32, bf16 = jnp.float32, jnp.bfloat16
    outs = (
        ((env_dev, hor_act), f32),
        ((env_dev, hor_act), f32),
        ((iters, cand_dev, env_dev), f32),
    )
    operands = (
        white.reshape(iters * rows, flat),
        mean_init,
        std_init,
        init_state,
        goal_state,
        w_state,
        w_action,
        w_out,
        bias_in.reshape(1, hidden),
        bias_out.reshape(1, state_dim),
        jnp.transpose(elite_idx, (1, 2, 0)),
        color_rows(flat // act, act).reshape(-1, WIDE // act, WIDE),
    )
    fmean, fstd, cost = pl.pallas_call(
        functools.partial(plan_kernel, dims),
        out_shape=tuple(pltpu.VMEM(shape, kind) for shape, kind in outs),
        in_specs=[hbm] * len(operands),
        out_specs=(vmem, vmem, vmem),
        scratch_shapes=[
            *(pltpu.VMEM(operand.shape, operand.dtype) for operand in operands),
            pltpu.VMEM((table_rows, WIDE), bf16),
            pltpu.VMEM((tiles, iters * rows, LANES), f32),
            pltpu.VMEM((iters, tiles, rows, LANES), bf16),
            pltpu.VMEM((LANES // act, state_dim + LANES, hidden), bf16),
            pltpu.VMEM((iters, rows, state_dim), f32),
            pltpu.VMEM((rows, state_dim), f32),
            pltpu.VMEM((iters, rows, LANES), f32),
            pltpu.VMEM((iters, cand_dev, env_dev, LANES), f32),
            pltpu.VMEM((units, SUB, LANES), f32),
            pltpu.VMEM((units, SUB, LANES), f32),
            pltpu.VMEM((iters, units, 2, SUB, LANES), f32),
            pltpu.VMEM((iters, n_cand - 1, share, 2, SUB, LANES), f32),
            pltpu.VMEM((iters, units, 2, SUB, LANES), f32),
            pltpu.VMEM((iters, 1, LANES), f32),
            pltpu.VMEM((iters, n_cand * n_env, 1, LANES), f32),
            pltpu.SemaphoreType.DMA((len(operands) + 1,)),
            pltpu.SemaphoreType.DMA((iters, 5)),
            pltpu.SemaphoreType.DMA((iters, 5)),
        ],
        compiler_params=pltpu.CompilerParams(collective_id=0, has_side_effects=True),
    )(*operands)
    fmean, fstd, cost = pl.pallas_call(
        store_kernel,
        out_shape=tuple(jax.ShapeDtypeStruct(shape, kind) for shape, kind in outs),
        in_specs=[vmem] * len(outs),
        out_specs=(hbm, hbm, hbm),
        scratch_shapes=[pltpu.SemaphoreType.DMA((len(outs),))],
    )(*(pltpu.with_memory_space_constraint(x, pltpu.VMEM) for x in (fmean, fstd, cost)))
    return fmean, fstd, jnp.swapaxes(cost, 1, 2)


def solution(mesh):
    in_specs = (
        P(None, "env", "cand", None),
        P("env", None),
        P("env", None),
        P("env", None),
        P("env", None),
        P(),
        P(),
        P(),
        P(),
        P(),
        P("env", None, None),
    )
    out_specs = (P("env", None), P("env", None), P(None, "env", "cand"))
    return jax.shard_map(shards, mesh=mesh, in_specs=in_specs, out_specs=out_specs, check_vma=False)
```

```python
import functools

import jax
import jax.numpy as jnp
import numpy as np
from jax import lax
from jax.experimental import pallas as pl
from jax.experimental.pallas import tpu as pltpu
from jax.sharding import PartitionSpec as P

BETA_EXP = 2.5
MOMENTUM = 0.1
FLOOR_SHARE = 0.1
ACT_COST = 0.1
MESH = pl.DeviceIdType.MESH
LANES = 128
WIDE = 256
SUB = 8

TRIPS = 10
WHILE_EARLY = (
    ((((0, 0),), 2, 1, (1, 0)),),
    ((((0, 6), (1, 0)), 2, 1, (2, 0)),),
    ((((2, 0), (1, 6)), 1, 2, None), (((2, 2), (1, 8)), 1, 2, None)),
)
WHILE_LATE = ((), (), ())
WHILE_PEAKS = (
    ((((0, 2),), 3, 1, (1, 4)), (((0, 5),), 1, 1, None)),
    ((((0, 8), (1, 2)), 2, 1, (2, 4)), (((1, 4),), 1, 1, (2, 8)), (((1, 5),), 1, 1, None)),
    ((((2, 4),), 1, 2, None), (((2, 6),), 1, 2, None), (((2, 8),), 1, 2, None)),
)


def color_rows(length, act):
    freqs = np.arange(length // 2 + 1)
    scale = (np.maximum(freqs, 1) / length) ** (-BETA_EXP / 2)
    kernel = np.fft.irfft(scale, n=length)
    kernel = kernel / np.sqrt(np.sum(kernel * kernel))
    q = WIDE // act
    row = np.arange(length)
    lane_step = np.arange(WIDE) // act
    shift = (q * (row // q))[:, None] + lane_step[None, :] - (row % q)[:, None]
    return jnp.asarray(kernel[shift % length], dtype=jnp.bfloat16).astype(jnp.float32)


def plan_kernel(
    dims,
    white_hbm,
    mean_hbm,
    std_hbm,
    start_hbm,
    goal_hbm,
    ws_hbm,
    wa_hbm,
    wo_hbm,
    bi_hbm,
    bo_hbm,
    elite_hbm,
    color_hbm,
    fmean_ref,
    fstd_ref,
    cost_out,
    white,
    mean_ref,
    std_ref,
    start_ref,
    goal_ref,
    ws_ref,
    wa_ref,
    wo_ref,
    bi_ref,
    bo_ref,
    elite_ref,
    color_ref,
    table,
    noise,
    acts,
    w_pair,
    state,
    goals,
    cost,
    member,
    cen,
    spr,
    part,
    rs_recv,
    ag,
    z_send,
    z_recv,
    copy_sem,
    send_sem,
    recv_sem,
):
    iters, env_dev, cand_dev, act, tiles, units, share, n_cand, n_env, elites = dims
    rows = env_dev * cand_dev
    state_dim = start_ref.shape[1]
    halves = env_dev // SUB
    n_units = tiles * halves
    n_all = n_cand * n_env
    length_blocks = white.shape[1] // WIDE
    out_blocks = tiles * LANES // WIDE
    low_block = length_blocks - out_blocks + 1
    per_tile = LANES // act
    me = lax.axis_index("cand")
    me_env = lax.axis_index("env")

    pairs = (
        (color_hbm, color_ref),
        (white_hbm.at[pl.ds(0, rows)], white.at[pl.ds(0, rows)]),
        (elite_hbm, elite_ref),
        (mean_hbm, mean_ref),
        (std_hbm, std_ref),
        (start_hbm, start_ref),
        (goal_hbm, goal_ref),
        (ws_hbm, ws_ref),
        (wa_hbm, wa_ref),
        (wo_hbm, wo_ref),
        (bi_hbm, bi_ref),
        (bo_hbm, bo_ref),
        (
            white_hbm.at[pl.ds(rows, (iters - 1) * rows)],
            white.at[pl.ds(rows, (iters - 1) * rows)],
        ),
    )
    loads = [
        pltpu.make_async_copy(src, dst, copy_sem.at[at]) for at, (src, dst) in enumerate(pairs)
    ]
    for load in loads[:-1]:
        load.start()

    def peer_of(k):
        return {
            "env": lax.rem(me_env + k // n_cand, n_env),
            "cand": lax.rem(me + k % n_cand, n_cand),
        }

    def every_peer(visit):
        if n_all <= 64:
            for k in range(n_all - 1, 0, -1):
                visit(k)
        else:
            lax.fori_loop(1, n_all, lambda k, carry: (visit(k), carry)[1], 0)

    barrier = pltpu.get_barrier_semaphore()
    for axis, place, number in (("cand", me, n_cand), ("env", me_env, n_env)):
        for o in range(1, number):
            other = {axis: lax.rem(place + o, number)}
            pl.semaphore_signal(barrier, inc=1, device_id=other, device_id_type=MESH)

    q = WIDE // act
    eye = (
        lax.broadcasted_iota(jnp.int32, (act, WIDE), 0)
        == lax.broadcasted_iota(jnp.int32, (act, WIDE), 1) % act
    )

    def build(places, block, carry):
        shift = lax.rem(2 * length_blocks - (block + low_block), length_blocks)
        for j in range(q):
            line = color_ref[shift, j : j + 1, :]
            piece = jnp.where(eye, line, 0.0).astype(jnp.bfloat16)
            for place in places:
                start = pl.multiple_of((block + place) * WIDE + j * act, act)
                table[pl.ds(start, act), :] = piece
        return carry

    diagonal = lax.broadcasted_iota(jnp.int32, (env_dev, env_dev), 0) == lax.broadcasted_iota(
        jnp.int32, (env_dev, env_dev), 1
    )

    def mark_elites(it):
        own = elite_ref[it]
        for c in range(cand_dev):
            hit = (own == me * cand_dev + c).astype(jnp.float32)
            hit = jnp.sum(hit, axis=0, keepdims=True)
            hit = jnp.sum(jnp.where(diagonal, hit, 0.0), axis=1, keepdims=True)
            member[it, c] = jnp.broadcast_to(hit, (env_dev, LANES))

    def set_first():
        for load in loads[2:5]:
            load.wait()
        mark_elites(0)
        cost[...] = jnp.zeros_like(cost)
        if units > n_units:
            cen[...] = jnp.zeros_like(cen)
            spr[...] = jnp.zeros_like(spr)
            part[...] = jnp.zeros_like(part)
        for tile in range(tiles):
            for h in range(halves):
                at = (slice(h * SUB, (h + 1) * SUB), slice(tile * LANES, (tile + 1) * LANES))
                cen[tile * halves + h] = mean_ref[at]
                spr[tile * halves + h] = std_ref[at]

    def set_rest():
        for load in loads[5:]:
            load.wait()
        w_pair[...] = jnp.zeros_like(w_pair)
        for p in range(per_tile):
            w_pair[p, :state_dim, :] = ws_ref[...] * jnp.bfloat16(0.5)
            w_pair[p, state_dim + p * act : state_dim + (p + 1) * act, :] = wa_ref[...] * jnp.bfloat16(0.5)
        for it in range(1, iters):
            mark_elites(it)
        for c in range(cand_dev):
            spot = slice(c * env_dev, (c + 1) * env_dev)
            goals[spot, :] = goal_ref[...]
            for it in range(iters):
                state[it, spot, :] = start_ref[...]

    n_blocks = table.shape[0] // WIDE
    twice = min(max(n_blocks - length_blocks, 0), length_blocks)
    loads[0].wait()
    lax.fori_loop(0, twice, functools.partial(build, (0, length_blocks)), 0)
    lax.fori_loop(twice, min(length_blocks, n_blocks), functools.partial(build, (0,)), 0)
    loads[-1].start()
    set_first()

    def color_block(it, block):
        spot = pl.ds(it * rows, rows)
        start = pl.multiple_of((out_blocks - 1 - block) * WIDE, WIDE)
        band = table[pl.ds(start, white.shape[1]), :]
        out = jnp.dot(white[spot, :], band, preferred_element_type=jnp.float32)
        for p in range(WIDE // LANES):
            noise[block * (WIDE // LANES) + p, spot, :] = out[:, p * LANES : (p + 1) * LANES]

    def color_piece(it, block, piece, pieces):
        spot = pl.ds(it * rows, rows)
        width = white.shape[1] // pieces
        start = pl.multiple_of((out_blocks - 1 - block) * WIDE + piece * width, WIDE)
        band = table[pl.ds(start, width), :]
        taken = white[spot, piece * width : (piece + 1) * width]
        out = jnp.dot(taken, band, preferred_element_type=jnp.float32)
        for p in range(WIDE // LANES):
            half = out[:, p * LANES : (p + 1) * LANES]
            at = block * (WIDE // LANES) + p
            noise[at, spot, :] = half if piece == 0 else noise[at, spot, :] + half

    def color(it, first, count, group):
        def one(step, carry):
            for g in range(group):
                color_block(it, first + step * group + g)
            return carry

        lax.fori_loop(0, count // group, one, 0)

    act_weight = ACT_COST * state_dim / act

    def model(it, unit, scales):
        if it == 0:
            return cen[unit], spr[unit]
        floor, gain = scales
        return ag[it - 1, unit, 0], jnp.maximum(ag[it - 1, unit, 1], floor) * gain

    def make_actions(it, scales, first, count):
        def one(tile, carry):
            fitted = [model(it, tile * halves + h, scales) for h in range(halves)]
            center = jnp.concatenate([f[0] for f in fitted], axis=0)
            spread = jnp.concatenate([f[1] for f in fitted], axis=0)
            sums = jnp.zeros((env_dev, LANES), jnp.float32)
            squares = jnp.zeros((env_dev, LANES), jnp.float32)
            for c in range(cand_dev):
                drawn = noise[tile, pl.ds(it * rows + c, env_dev, stride=cand_dev), :]
                action = jnp.clip(center + spread * drawn, -1.0, 1.0)
                spot = slice(c * env_dev, (c + 1) * env_dev)
                acts[it, tile, spot, :] = action.astype(jnp.bfloat16)
                chosen = member[it, c] * action
                square = action * action
                sums = sums + chosen
                squares = squares + chosen * action
                cost[it, spot, :] += act_weight * square
            sums = sums.reshape(halves, SUB, LANES)
            squares = squares.reshape(halves, SUB, LANES)
            for h in range(halves):
                part[it, tile * halves + h, 0] = sums[h]
                part[it, tile * halves + h, 1] = squares[h]
            return carry

        lax.fori_loop(first, first + count, one, 0)

    lots = ((0, share // 2), (share // 2, share - share // 2)) if share > 1 else ((0, share),)
    sums_stage, means_stage, peaks_stage = 0, len(lots), 2 * len(lots)

    def split(parts):
        even = units == n_units and n_cand % parts == 0 and tiles % parts == 0
        return parts if even else 1

    def send_to(it, peer, slot, lot):
        low, size = lots[lot]
        pltpu.make_async_remote_copy(
            src_ref=part.at[it, pl.ds(peer * share + low, size)],
            dst_ref=rs_recv.at[it, slot, pl.ds(low, size)],
            send_sem=send_sem.at[it, sums_stage + lot],
            recv_sem=recv_sem.at[it, sums_stage + lot],
            device_id={"cand": peer},
            device_id_type=MESH,
        ).start()

    def send_sums(it, parts, k, lot):
        crowd = n_cand // parts
        near = int(k == parts - 1)
        at = lax.rem(me // crowd + 1 + k, parts)
        for o in range(near, crowd):
            peer = at * crowd + lax.rem(lax.rem(me, crowd) + o, crowd)
            send_to(it, peer, k * crowd + o - near, lot)

    def send_means(it, lot):
        low, size = lots[lot]
        mine = ag.at[it, pl.ds(me * share + low, size)]
        for o in range(1, n_cand):
            pltpu.make_async_remote_copy(
                src_ref=mine,
                dst_ref=mine,
                send_sem=send_sem.at[it, means_stage + lot],
                recv_sem=recv_sem.at[it, means_stage + lot],
                device_id={"cand": lax.rem(me + o, n_cand)},
                device_id_type=MESH,
            ).start()

    def send_peaks(it):
        every_peer(
            lambda k: pltpu.make_async_remote_copy(
                src_ref=z_send.at[it],
                dst_ref=z_recv.at[it, k],
                send_sem=send_sem.at[it, peaks_stage],
                recv_sem=recv_sem.at[it, peaks_stage],
                device_id=peer_of(k),
                device_id_type=MESH,
            ).start()
        )

    def await_bytes(stage, it, sem):
        if stage == peaks_stage:
            ref = z_recv.at[it, pl.ds(1, n_all - 1)]
        elif stage < means_stage:
            low, size = lots[stage]
            ref = rs_recv.at[it, pl.ds(0, n_cand - 1), pl.ds(low, size)]
        else:
            ref = ag.at[it, pl.ds(0, (n_cand - 1) * lots[stage - means_stage][1])]
        pltpu.make_async_copy(ref, ref, sem.at[it, stage]).wait()

    def refit(it, scales, lot):
        low, size = lots[lot]
        await_bytes(sums_stage + lot, it, recv_sem)
        mine = pl.ds(me * share + low, size)
        total = part[it, mine] + jnp.sum(rs_recv[it, :, low : low + size], axis=0)
        mean = total[:, 0] / elites
        deviation = jnp.sqrt(jnp.maximum(total[:, 1] / elites - mean * mean, 0.0))
        center, spread = model(it, mine, scales)
        mixed = MOMENTUM * spread + (1.0 - MOMENTUM) * deviation
        ag[it, mine, 0] = MOMENTUM * center + (1.0 - MOMENTUM) * mean
        ag[it, mine, 1] = mixed
        lane = lax.broadcasted_iota(jnp.int32, (SUB, LANES), 1)
        sub = lax.broadcasted_iota(jnp.int32, (SUB, LANES), 0)
        row = jnp.zeros((SUB, LANES), jnp.float32)
        for i in range(size):
            half = lax.rem(me * share + low + i, halves)
            best = jnp.max(mixed[i], axis=1, keepdims=True)
            row = jnp.maximum(row, jnp.where(lane == half * SUB + sub, best, 0.0))
        row = jnp.max(row, axis=0, keepdims=True)
        if lot:
            row = jnp.maximum(row, z_send[it])
        z_send[it] = row
        if lot == len(lots) - 1:
            z_recv[it, 0] = row
            send_peaks(it)
        send_means(it, lot)

    def settle(it):
        await_bytes(peaks_stage, it, recv_sem)
        peaks = jnp.max(z_recv[it].reshape(n_env, n_cand, 1, LANES), axis=1)
        peak = jnp.max(jnp.max(peaks, axis=0), axis=1, keepdims=True)
        settled = jnp.sum(jnp.sum(peaks, axis=0), axis=1, keepdims=True) / peak / (env_dev * n_env)
        floor = jnp.broadcast_to(FLOOR_SHARE * peak, (SUB, LANES))
        gain = jnp.broadcast_to(0.5 + settled, (SUB, LANES))
        for lot in range(len(lots)):
            await_bytes(means_stage + lot, it, recv_sem)
        return floor, gain

    per_trip = -(-tiles // TRIPS)

    def rollout(chains, count, span, paint):
        bias_h = bi_ref[...] * 0.5
        bias_o = bo_ref[...]
        its = [it for it, _ in chains]

        def steps(i, carry):
            pieces = span * per_trip * per_tile
            for s in range(pieces):
                tile, p = s // per_tile, s % per_tile
                hidden = []
                for it, low in chains:
                    action = acts[it, (low + i * span) * per_trip + tile]
                    x = jnp.concatenate([state[it].astype(jnp.bfloat16), action], axis=1)
                    h = jnp.dot(x, w_pair[p], preferred_element_type=jnp.float32) + bias_h
                    hidden.append((h * jnp.tanh(h) + h).astype(jnp.bfloat16))
                if paint is not None:
                    color_piece(paint[0], paint[1] + i * 2, s, pieces)
                for it, hid in zip(its, hidden):
                    delta = jnp.dot(hid, wo_ref[...], preferred_element_type=jnp.float32)
                    then = jnp.tanh((state[it] + bias_o) + delta)
                    error = then - goals[...]
                    cost[it] += error * error
                    state[it] = then
                if paint is not None:
                    color_piece(paint[0], paint[1] + i * 2 + 1, s, pieces)
            return carry

        lax.fori_loop(0, count, steps, 0)

    def work(groups):
        for chains, count, span, paint in groups:
            rollout(chains, count, span, paint)

    everything = range(len(lots))

    def open_far(half):
        crowd, some = n_cand // 2, tiles // 2
        size = half + half % 2
        early = size - 2
        early_tiles = early * (WIDE // LANES)
        served = early_tiles * halves // share
        at = 1 - me // crowd
        mine = lax.rem(me, crowd)
        color(0, at * (out_blocks - early), early, early)
        make_actions(0, None, at * (tiles - early_tiles), early_tiles)
        pl.semaphore_wait(barrier, n_cand - 1 + n_env - 1)
        for j in range(served):
            rank = at * (crowd - served) + lax.rem(mine + j, served)
            for lot in everything:
                send_to(0, at * crowd + rank, lax.rem(rank - mine + crowd, crowd), lot)
        color(0, early + at * (out_blocks - 2 * early - 2), 2, 2)
        make_actions(0, None, early_tiles + at * (some - early_tiles), some - early_tiles)
        for j in range(crowd - served):
            rank = (1 - at) * served + j
            for lot in everything:
                send_to(0, at * crowd + rank, lax.rem(rank - mine + crowd, crowd), lot)

    loads[1].wait()
    scales = None
    for it in range(iters):
        parts = split(4 if it else 2)
        count = tiles // parts
        for k in range(parts):
            at = lax.rem(me // (n_cand // parts) + 1 + k, parts)
            if it == 0:
                half = out_blocks // parts
                if parts == 2 and k == 0 and half > 2:
                    open_far(half)
                    continue
                size = half - half % 2 if parts == 2 and half > 2 else half
                color(0, at * (out_blocks - size), size, size)
            make_actions(it, scales, at * count, count)
            if it == 0 and k == 0:
                pl.semaphore_wait(barrier, n_cand - 1 + n_env - 1)
            for lot in everything if it == 0 or parts == 1 else (0,):
                send_sums(it, parts, k, lot)
        if it and parts > 1:
            for k in range(parts):
                for lot in everything[1:]:
                    send_sums(it, parts, k, lot)
        if it == 0:
            set_rest()
        work(WHILE_EARLY[it])
        if len(lots) > 1:
            refit(it, scales, 0)
        work(WHILE_LATE[it])
        refit(it, scales, len(lots) - 1)
        work(WHILE_PEAKS[it])
        if it == iters - 1:
            scale = 1.0 / (state_dim * tiles * per_tile)
            for i in range(iters):
                for c in range(cand_dev):
                    total = jnp.sum(cost[i, c * env_dev : (c + 1) * env_dev, :], axis=1, keepdims=True)
                    line = jnp.sum(jnp.where(diagonal, total * scale, 0.0), axis=0, keepdims=True)
                    cost_out[i, c : c + 1, :] = line
        scales = settle(it)

    for tile in range(tiles):
        for h in range(halves):
            at = (slice(h * SUB, (h + 1) * SUB), slice(tile * LANES, (tile + 1) * LANES))
            fmean_ref[at], fstd_ref[at] = model(iters, tile * halves + h, scales)
    for it in range(iters):
        for stage in range(peaks_stage + 1):
            await_bytes(stage, it, send_sem)


def store_kernel(fmean_ref, fstd_ref, cost_ref, fmean_hbm, fstd_hbm, cost_hbm, sem):
    copies = [
        pltpu.make_async_copy(src, dst, sem.at[at])
        for at, (src, dst) in enumerate(
            ((fmean_ref, fmean_hbm), (fstd_ref, fstd_hbm), (cost_ref, cost_hbm))
        )
    ]
    for copy in copies:
        copy.start()
    for copy in copies:
        copy.wait()


def shards(
    white,
    mean_init,
    std_init,
    init_state,
    goal_state,
    w_state,
    w_action,
    w_out,
    bias_in,
    bias_out,
    elite_idx,
):
    iters, env_dev, cand_dev, flat = white.shape
    act, hidden = w_action.shape
    state_dim = w_state.shape[0]
    hor_act = mean_init.shape[1]
    n_cand = lax.axis_size("cand")
    n_env = lax.axis_size("env")
    tiles = hor_act // LANES
    halves = env_dev // SUB
    share = -(-tiles * halves // n_cand)
    units = share * n_cand
    rows = env_dev * cand_dev
    out_blocks = hor_act // WIDE
    table_rows = flat + (out_blocks - 1) * WIDE
    dims = (iters, env_dev, cand_dev, act, tiles, units, share, n_cand, n_env, elite_idx.shape[2])
    hbm = pl.BlockSpec(memory_space=pl.ANY)
    vmem = pl.BlockSpec(memory_space=pltpu.VMEM)
    f32, bf16 = jnp.float32, jnp.bfloat16
    outs = (
        ((env_dev, hor_act), f32),
        ((env_dev, hor_act), f32),
        ((iters, cand_dev, env_dev), f32),
    )
    operands = (
        white.reshape(iters * rows, flat),
        mean_init,
        std_init,
        init_state,
        goal_state,
        w_state,
        w_action,
        w_out,
        bias_in.reshape(1, hidden),
        bias_out.reshape(1, state_dim),
        jnp.transpose(elite_idx, (1, 2, 0)),
        color_rows(flat // act, act).reshape(-1, WIDE // act, WIDE),
    )
    fmean, fstd, cost = pl.pallas_call(
        functools.partial(plan_kernel, dims),
        out_shape=tuple(pltpu.VMEM(shape, kind) for shape, kind in outs),
        in_specs=[hbm] * len(operands),
        out_specs=(vmem, vmem, vmem),
        scratch_shapes=[
            *(pltpu.VMEM(operand.shape, operand.dtype) for operand in operands),
            pltpu.VMEM((table_rows, WIDE), bf16),
            pltpu.VMEM((tiles, iters * rows, LANES), f32),
            pltpu.VMEM((iters, tiles, rows, LANES), bf16),
            pltpu.VMEM((LANES // act, state_dim + LANES, hidden), bf16),
            pltpu.VMEM((iters, rows, state_dim), f32),
            pltpu.VMEM((rows, state_dim), f32),
            pltpu.VMEM((iters, rows, LANES), f32),
            pltpu.VMEM((iters, cand_dev, env_dev, LANES), f32),
            pltpu.VMEM((units, SUB, LANES), f32),
            pltpu.VMEM((units, SUB, LANES), f32),
            pltpu.VMEM((iters, units, 2, SUB, LANES), f32),
            pltpu.VMEM((iters, n_cand - 1, share, 2, SUB, LANES), f32),
            pltpu.VMEM((iters, units, 2, SUB, LANES), f32),
            pltpu.VMEM((iters, 1, LANES), f32),
            pltpu.VMEM((iters, n_cand * n_env, 1, LANES), f32),
            pltpu.SemaphoreType.DMA((len(operands) + 1,)),
            pltpu.SemaphoreType.DMA((iters, 5)),
            pltpu.SemaphoreType.DMA((iters, 5)),
        ],
        compiler_params=pltpu.CompilerParams(collective_id=0, has_side_effects=True),
    )(*operands)
    fmean, fstd, cost = pl.pallas_call(
        store_kernel,
        out_shape=tuple(jax.ShapeDtypeStruct(shape, kind) for shape, kind in outs),
        in_specs=[vmem] * len(outs),
        out_specs=(hbm, hbm, hbm),
        scratch_shapes=[pltpu.SemaphoreType.DMA((len(outs),))],
    )(*(pltpu.with_memory_space_constraint(x, pltpu.VMEM) for x in (fmean, fstd, cost)))
    return fmean, fstd, jnp.swapaxes(cost, 1, 2)


def solution(mesh):
    in_specs = (
        P(None, "env", "cand", None),
        P("env", None),
        P("env", None),
        P("env", None),
        P("env", None),
        P(),
        P(),
        P(),
        P(),
        P(),
        P("env", None, None),
    )
    out_specs = (P("env", None), P("env", None), P(None, "env", "cand"))
    return jax.shard_map(shards, mesh=mesh, in_specs=in_specs, out_specs=out_specs, check_vma=False)
```

```python
import functools

import jax
import jax.numpy as jnp
import numpy as np
from jax import lax
from jax.experimental import pallas as pl
from jax.experimental.pallas import tpu as pltpu
from jax.sharding import PartitionSpec as P

BETA_EXP = 2.5
MOMENTUM = 0.1
FLOOR_SHARE = 0.1
ACT_COST = 0.1
MESH = pl.DeviceIdType.MESH
LANES = 128
WIDE = 256
SUB = 8

TRIPS = 10
WHILE_EARLY = (
    ((((0, 0),), 2, 1, (1, 0)),),
    ((((0, 5), (1, 0)), 2, 1, (2, 0)),),
    ((((2, 0), (1, 5)), 1, 2, None), (((2, 2), (1, 7)), 1, 2, None)),
)
WHILE_LATE = (
    (),
    (),
    (),
)
WHILE_PEAKS = (
    ((((0, 2),), 3, 1, (1, 4)),),
    ((((0, 7), (1, 2)), 3, 1, (2, 4)),),
    ((((2, 4), (1, 9)), 1, 1, None), (((2, 5),), 1, 1, None), (((2, 6),), 1, 2, None), (((2, 8),), 1, 2, None)),
)


def color_rows(length, act):
    freqs = np.arange(length // 2 + 1)
    scale = (np.maximum(freqs, 1) / length) ** (-BETA_EXP / 2)
    kernel = np.fft.irfft(scale, n=length)
    kernel = kernel / np.sqrt(np.sum(kernel * kernel))
    q = WIDE // act
    row = np.arange(length)
    lane_step = np.arange(WIDE) // act
    shift = (q * (row // q))[:, None] + lane_step[None, :] - (row % q)[:, None]
    return jnp.asarray(kernel[shift % length], dtype=jnp.bfloat16).astype(jnp.float32)


def plan_kernel(
    dims,
    white_hbm,
    mean_hbm,
    std_hbm,
    start_hbm,
    goal_hbm,
    ws_hbm,
    wa_hbm,
    wo_hbm,
    bi_hbm,
    bo_hbm,
    elite_hbm,
    color_hbm,
    fmean_ref,
    fstd_ref,
    cost_out,
    white,
    mean_ref,
    std_ref,
    start_ref,
    goal_ref,
    ws_ref,
    wa_ref,
    wo_ref,
    bi_ref,
    bo_ref,
    elite_ref,
    color_ref,
    table,
    noise,
    acts,
    w_pair,
    state,
    goals,
    cost,
    member,
    cen,
    spr,
    part,
    rs_recv,
    ag,
    z_send,
    z_recv,
    copy_sem,
    send_sem,
    recv_sem,
):
    iters, env_dev, cand_dev, act, tiles, units, share, n_cand, n_env, elites = dims
    rows = env_dev * cand_dev
    state_dim = start_ref.shape[1]
    halves = env_dev // SUB
    n_units = tiles * halves
    n_all = n_cand * n_env
    length_blocks = white.shape[1] // WIDE
    out_blocks = tiles * LANES // WIDE
    low_block = length_blocks - out_blocks + 1
    per_tile = LANES // act
    me = lax.axis_index("cand")
    me_env = lax.axis_index("env")

    pairs = (
        (color_hbm, color_ref),
        (white_hbm.at[pl.ds(0, rows)], white.at[pl.ds(0, rows)]),
        (elite_hbm, elite_ref),
        (mean_hbm, mean_ref),
        (std_hbm, std_ref),
        (start_hbm, start_ref),
        (goal_hbm, goal_ref),
        (ws_hbm, ws_ref),
        (wa_hbm, wa_ref),
        (wo_hbm, wo_ref),
        (bi_hbm, bi_ref),
        (bo_hbm, bo_ref),
        (
            white_hbm.at[pl.ds(rows, (iters - 1) * rows)],
            white.at[pl.ds(rows, (iters - 1) * rows)],
        ),
    )
    loads = [
        pltpu.make_async_copy(src, dst, copy_sem.at[at]) for at, (src, dst) in enumerate(pairs)
    ]
    for load in loads[:-1]:
        load.start()

    def peer_of(k):
        return {
            "env": lax.rem(me_env + k // n_cand, n_env),
            "cand": lax.rem(me + k % n_cand, n_cand),
        }

    def every_peer(visit):
        if n_all <= 64:
            for k in range(n_all - 1, 0, -1):
                visit(k)
        else:
            lax.fori_loop(1, n_all, lambda k, carry: (visit(k), carry)[1], 0)

    barrier = pltpu.get_barrier_semaphore()
    for axis, place, number in (("cand", me, n_cand), ("env", me_env, n_env)):
        for o in range(1, number):
            other = {axis: lax.rem(place + o, number)}
            pl.semaphore_signal(barrier, inc=1, device_id=other, device_id_type=MESH)

    q = WIDE // act
    eye = (
        lax.broadcasted_iota(jnp.int32, (act, WIDE), 0)
        == lax.broadcasted_iota(jnp.int32, (act, WIDE), 1) % act
    )

    def build(places, block, carry):
        shift = lax.rem(2 * length_blocks - (block + low_block), length_blocks)
        for j in range(q):
            line = color_ref[shift, j : j + 1, :]
            piece = jnp.where(eye, line, 0.0).astype(jnp.bfloat16)
            for place in places:
                start = pl.multiple_of((block + place) * WIDE + j * act, act)
                table[pl.ds(start, act), :] = piece
        return carry

    diagonal = lax.broadcasted_iota(jnp.int32, (env_dev, env_dev), 0) == lax.broadcasted_iota(
        jnp.int32, (env_dev, env_dev), 1
    )

    def mark_elites(it):
        own = elite_ref[it]
        for c in range(cand_dev):
            hit = (own == me * cand_dev + c).astype(jnp.float32)
            hit = jnp.sum(hit, axis=0, keepdims=True)
            hit = jnp.sum(jnp.where(diagonal, hit, 0.0), axis=1, keepdims=True)
            member[it, c] = jnp.broadcast_to(hit, (env_dev, LANES))

    def set_first():
        for load in loads[2:5]:
            load.wait()
        mark_elites(0)
        cost[...] = jnp.zeros_like(cost)
        if units > n_units:
            cen[...] = jnp.zeros_like(cen)
            spr[...] = jnp.zeros_like(spr)
            part[...] = jnp.zeros_like(part)
        for tile in range(tiles):
            for h in range(halves):
                at = (slice(h * SUB, (h + 1) * SUB), slice(tile * LANES, (tile + 1) * LANES))
                cen[tile * halves + h] = mean_ref[at]
                spr[tile * halves + h] = std_ref[at]

    def set_rest():
        for load in loads[5:]:
            load.wait()
        w_pair[...] = jnp.zeros_like(w_pair)
        for p in range(per_tile):
            w_pair[p, :state_dim, :] = ws_ref[...] * jnp.bfloat16(0.5)
            w_pair[p, state_dim + p * act : state_dim + (p + 1) * act, :] = wa_ref[...] * jnp.bfloat16(0.5)
        for it in range(1, iters):
            mark_elites(it)
        for c in range(cand_dev):
            spot = slice(c * env_dev, (c + 1) * env_dev)
            goals[spot, :] = goal_ref[...]
            for it in range(iters):
                state[it, spot, :] = start_ref[...]

    n_blocks = table.shape[0] // WIDE
    twice = min(max(n_blocks - length_blocks, 0), length_blocks)
    loads[0].wait()
    lax.fori_loop(0, twice, functools.partial(build, (0, length_blocks)), 0)
    lax.fori_loop(twice, min(length_blocks, n_blocks), functools.partial(build, (0,)), 0)
    loads[-1].start()
    set_first()

    def color_block(it, block):
        spot = pl.ds(it * rows, rows)
        start = pl.multiple_of((out_blocks - 1 - block) * WIDE, WIDE)
        band = table[pl.ds(start, white.shape[1]), :]
        out = jnp.dot(white[spot, :], band, preferred_element_type=jnp.float32)
        for p in range(WIDE // LANES):
            noise[block * (WIDE // LANES) + p, spot, :] = out[:, p * LANES : (p + 1) * LANES]

    def color_piece(it, block, piece, pieces):
        spot = pl.ds(it * rows, rows)
        width = white.shape[1] // pieces
        start = pl.multiple_of((out_blocks - 1 - block) * WIDE + piece * width, WIDE)
        band = table[pl.ds(start, width), :]
        taken = white[spot, piece * width : (piece + 1) * width]
        out = jnp.dot(taken, band, preferred_element_type=jnp.float32)
        for p in range(WIDE // LANES):
            half = out[:, p * LANES : (p + 1) * LANES]
            at = block * (WIDE // LANES) + p
            noise[at, spot, :] = half if piece == 0 else noise[at, spot, :] + half

    def color(it, first, count, group):
        def one(step, carry):
            for g in range(group):
                color_block(it, first + step * group + g)
            return carry

        lax.fori_loop(0, count // group, one, 0)

    act_weight = ACT_COST * state_dim / act

    def model(it, unit, scales):
        if it == 0:
            return cen[unit], spr[unit]
        floor, gain = scales
        return ag[it - 1, unit, 0], jnp.maximum(ag[it - 1, unit, 1], floor) * gain

    def make_actions(it, scales, first, count):
        def one(tile, carry):
            fitted = [model(it, tile * halves + h, scales) for h in range(halves)]
            center = jnp.concatenate([f[0] for f in fitted], axis=0)
            spread = jnp.concatenate([f[1] for f in fitted], axis=0)
            sums = jnp.zeros((env_dev, LANES), jnp.float32)
            squares = jnp.zeros((env_dev, LANES), jnp.float32)
            for c in range(cand_dev):
                drawn = noise[tile, pl.ds(it * rows + c, env_dev, stride=cand_dev), :]
                action = jnp.clip(center + spread * drawn, -1.0, 1.0)
                spot = slice(c * env_dev, (c + 1) * env_dev)
                acts[it, tile, spot, :] = action.astype(jnp.bfloat16)
                chosen = member[it, c] * action
                square = action * action
                sums = sums + chosen
                squares = squares + chosen * action
                cost[it, spot, :] += act_weight * square
            sums = sums.reshape(halves, SUB, LANES)
            squares = squares.reshape(halves, SUB, LANES)
            for h in range(halves):
                part[it, tile * halves + h, 0] = sums[h]
                part[it, tile * halves + h, 1] = squares[h]
            return carry

        lax.fori_loop(first, first + count, one, 0)

    lots = ((0, share // 2), (share // 2, share - share // 2)) if share > 1 else ((0, share),)
    sums_stage, means_stage, peaks_stage = 0, len(lots), 2 * len(lots)

    def split(parts):
        even = units == n_units and n_cand % parts == 0 and tiles % parts == 0
        return parts if even else 1

    def send_to(it, peer, slot, lot):
        low, size = lots[lot]
        pltpu.make_async_remote_copy(
            src_ref=part.at[it, pl.ds(peer * share + low, size)],
            dst_ref=rs_recv.at[it, slot, pl.ds(low, size)],
            send_sem=send_sem.at[it, sums_stage + lot],
            recv_sem=recv_sem.at[it, sums_stage + lot],
            device_id={"cand": peer},
            device_id_type=MESH,
        ).start()

    def send_sums(it, parts, k, lot):
        crowd = n_cand // parts
        near = int(k == parts - 1)
        at = lax.rem(me // crowd + 1 + k, parts)
        for o in range(near, crowd):
            peer = at * crowd + lax.rem(lax.rem(me, crowd) + o, crowd)
            send_to(it, peer, k * crowd + o - near, lot)

    def send_means(it, lot):
        low, size = lots[lot]
        mine = ag.at[it, pl.ds(me * share + low, size)]
        for o in range(1, n_cand):
            pltpu.make_async_remote_copy(
                src_ref=mine,
                dst_ref=mine,
                send_sem=send_sem.at[it, means_stage + lot],
                recv_sem=recv_sem.at[it, means_stage + lot],
                device_id={"cand": lax.rem(me + o, n_cand)},
                device_id_type=MESH,
            ).start()

    def send_peaks(it):
        every_peer(
            lambda k: pltpu.make_async_remote_copy(
                src_ref=z_send.at[it],
                dst_ref=z_recv.at[it, k],
                send_sem=send_sem.at[it, peaks_stage],
                recv_sem=recv_sem.at[it, peaks_stage],
                device_id=peer_of(k),
                device_id_type=MESH,
            ).start()
        )

    def await_bytes(stage, it, sem):
        if stage == peaks_stage:
            ref = z_recv.at[it, pl.ds(1, n_all - 1)]
        elif stage < means_stage:
            low, size = lots[stage]
            ref = rs_recv.at[it, pl.ds(0, n_cand - 1), pl.ds(low, size)]
        else:
            ref = ag.at[it, pl.ds(0, (n_cand - 1) * lots[stage - means_stage][1])]
        pltpu.make_async_copy(ref, ref, sem.at[it, stage]).wait()

    def refit(it, scales, lot):
        low, size = lots[lot]
        await_bytes(sums_stage + lot, it, recv_sem)
        mine = pl.ds(me * share + low, size)
        total = part[it, mine] + jnp.sum(rs_recv[it, :, low : low + size], axis=0)
        mean = total[:, 0] / elites
        deviation = jnp.sqrt(jnp.maximum(total[:, 1] / elites - mean * mean, 0.0))
        center, spread = model(it, mine, scales)
        mixed = MOMENTUM * spread + (1.0 - MOMENTUM) * deviation
        ag[it, mine, 0] = MOMENTUM * center + (1.0 - MOMENTUM) * mean
        ag[it, mine, 1] = mixed
        lane = lax.broadcasted_iota(jnp.int32, (SUB, LANES), 1)
        sub = lax.broadcasted_iota(jnp.int32, (SUB, LANES), 0)
        row = jnp.zeros((SUB, LANES), jnp.float32)
        for i in range(size):
            half = lax.rem(me * share + low + i, halves)
            best = jnp.max(mixed[i], axis=1, keepdims=True)
            row = jnp.maximum(row, jnp.where(lane == half * SUB + sub, best, 0.0))
        row = jnp.max(row, axis=0, keepdims=True)
        if lot:
            row = jnp.maximum(row, z_send[it])
        z_send[it] = row
        if lot == len(lots) - 1:
            z_recv[it, 0] = row
            send_peaks(it)
        send_means(it, lot)

    def settle(it):
        await_bytes(peaks_stage, it, recv_sem)
        peaks = jnp.max(z_recv[it].reshape(n_env, n_cand, 1, LANES), axis=1)
        peak = jnp.max(jnp.max(peaks, axis=0), axis=1, keepdims=True)
        settled = jnp.sum(jnp.sum(peaks, axis=0), axis=1, keepdims=True) / peak / (env_dev * n_env)
        floor = jnp.broadcast_to(FLOOR_SHARE * peak, (SUB, LANES))
        gain = jnp.broadcast_to(0.5 + settled, (SUB, LANES))
        for lot in range(len(lots)):
            await_bytes(means_stage + lot, it, recv_sem)
        return floor, gain

    per_trip = -(-tiles // TRIPS)

    def rollout(chains, count, span, paint):
        bias_h = bi_ref[...] * 0.5
        bias_o = bo_ref[...]
        its = [it for it, _ in chains]

        def steps(i, carry):
            pieces = span * per_trip * per_tile
            for s in range(pieces):
                tile, p = s // per_tile, s % per_tile
                hidden = []
                for it, low in chains:
                    action = acts[it, (low + i * span) * per_trip + tile]
                    x = jnp.concatenate([state[it].astype(jnp.bfloat16), action], axis=1)
                    h = jnp.dot(x, w_pair[p], preferred_element_type=jnp.float32) + bias_h
                    hidden.append((h * jnp.tanh(h) + h).astype(jnp.bfloat16))
                if paint is not None:
                    color_piece(paint[0], paint[1] + i * 2, s, pieces)
                for it, hid in zip(its, hidden):
                    delta = jnp.dot(hid, wo_ref[...], preferred_element_type=jnp.float32)
                    then = jnp.tanh((state[it] + bias_o) + delta)
                    error = then - goals[...]
                    cost[it] += error * error
                    state[it] = then
                if paint is not None:
                    color_piece(paint[0], paint[1] + i * 2 + 1, s, pieces)
            return carry

        lax.fori_loop(0, count, steps, 0)

    def work(groups):
        for chains, count, span, paint in groups:
            rollout(chains, count, span, paint)

    everything = range(len(lots))

    def open_far(half):
        crowd, some = n_cand // 2, tiles // 2
        size = half + half % 2
        early = size - 2
        early_tiles = early * (WIDE // LANES)
        served = early_tiles * halves // share
        at = 1 - me // crowd
        mine = lax.rem(me, crowd)
        color(0, at * (out_blocks - early), early, early)
        make_actions(0, None, at * (tiles - early_tiles), early_tiles)
        pl.semaphore_wait(barrier, n_cand - 1 + n_env - 1)
        for j in range(served):
            rank = at * (crowd - served) + lax.rem(mine + j, served)
            for lot in everything:
                send_to(0, at * crowd + rank, lax.rem(rank - mine + crowd, crowd), lot)
        color(0, early + at * (out_blocks - 2 * early - 2), 2, 2)
        make_actions(0, None, early_tiles + at * (some - early_tiles), some - early_tiles)
        for j in range(crowd - served):
            rank = (1 - at) * served + j
            for lot in everything:
                send_to(0, at * crowd + rank, lax.rem(rank - mine + crowd, crowd), lot)

    loads[1].wait()
    scales = None
    for it in range(iters):
        parts = split(4 if it else 2)
        count = tiles // parts
        for k in range(parts):
            at = lax.rem(me // (n_cand // parts) + 1 + k, parts)
            if it == 0:
                half = out_blocks // parts
                if parts == 2 and k == 0 and half > 2:
                    open_far(half)
                    continue
                size = half - half % 2 if parts == 2 and half > 2 else half
                color(0, at * (out_blocks - size), size, size)
            make_actions(it, scales, at * count, count)
            if it == 0 and k == 0:
                pl.semaphore_wait(barrier, n_cand - 1 + n_env - 1)
            for lot in everything if it == 0 or parts == 1 else (0,):
                send_sums(it, parts, k, lot)
        if it and parts > 1:
            for k in range(parts):
                for lot in everything[1:]:
                    send_sums(it, parts, k, lot)
        if it == 0:
            set_rest()
        work(WHILE_EARLY[it])
        if len(lots) > 1:
            refit(it, scales, 0)
        work(WHILE_LATE[it])
        refit(it, scales, len(lots) - 1)
        work(WHILE_PEAKS[it])
        if it == iters - 1:
            scale = 1.0 / (state_dim * tiles * per_tile)
            for i in range(iters):
                for c in range(cand_dev):
                    total = jnp.sum(cost[i, c * env_dev : (c + 1) * env_dev, :], axis=1, keepdims=True)
                    line = jnp.sum(jnp.where(diagonal, total * scale, 0.0), axis=0, keepdims=True)
                    cost_out[i, c : c + 1, :] = line
        scales = settle(it)

    for tile in range(tiles):
        for h in range(halves):
            at = (slice(h * SUB, (h + 1) * SUB), slice(tile * LANES, (tile + 1) * LANES))
            fmean_ref[at], fstd_ref[at] = model(iters, tile * halves + h, scales)
    for it in range(iters):
        for stage in range(peaks_stage + 1):
            await_bytes(stage, it, send_sem)


def store_kernel(fmean_ref, fstd_ref, cost_ref, fmean_hbm, fstd_hbm, cost_hbm, sem):
    copies = [
        pltpu.make_async_copy(src, dst, sem.at[at])
        for at, (src, dst) in enumerate(
            ((fmean_ref, fmean_hbm), (fstd_ref, fstd_hbm), (cost_ref, cost_hbm))
        )
    ]
    for copy in copies:
        copy.start()
    for copy in copies:
        copy.wait()


def shards(
    white,
    mean_init,
    std_init,
    init_state,
    goal_state,
    w_state,
    w_action,
    w_out,
    bias_in,
    bias_out,
    elite_idx,
):
    iters, env_dev, cand_dev, flat = white.shape
    act, hidden = w_action.shape
    state_dim = w_state.shape[0]
    hor_act = mean_init.shape[1]
    n_cand = lax.axis_size("cand")
    n_env = lax.axis_size("env")
    tiles = hor_act // LANES
    halves = env_dev // SUB
    share = -(-tiles * halves // n_cand)
    units = share * n_cand
    rows = env_dev * cand_dev
    out_blocks = hor_act // WIDE
    table_rows = flat + (out_blocks - 1) * WIDE
    dims = (iters, env_dev, cand_dev, act, tiles, units, share, n_cand, n_env, elite_idx.shape[2])
    hbm = pl.BlockSpec(memory_space=pl.ANY)
    vmem = pl.BlockSpec(memory_space=pltpu.VMEM)
    f32, bf16 = jnp.float32, jnp.bfloat16
    outs = (
        ((env_dev, hor_act), f32),
        ((env_dev, hor_act), f32),
        ((iters, cand_dev, env_dev), f32),
    )
    operands = (
        white.reshape(iters * rows, flat),
        mean_init,
        std_init,
        init_state,
        goal_state,
        w_state,
        w_action,
        w_out,
        bias_in.reshape(1, hidden),
        bias_out.reshape(1, state_dim),
        jnp.transpose(elite_idx, (1, 2, 0)),
        color_rows(flat // act, act).reshape(-1, WIDE // act, WIDE),
    )
    fmean, fstd, cost = pl.pallas_call(
        functools.partial(plan_kernel, dims),
        out_shape=tuple(pltpu.VMEM(shape, kind) for shape, kind in outs),
        in_specs=[hbm] * len(operands),
        out_specs=(vmem, vmem, vmem),
        scratch_shapes=[
            *(pltpu.VMEM(operand.shape, operand.dtype) for operand in operands),
            pltpu.VMEM((table_rows, WIDE), bf16),
            pltpu.VMEM((tiles, iters * rows, LANES), f32),
            pltpu.VMEM((iters, tiles, rows, LANES), bf16),
            pltpu.VMEM((LANES // act, state_dim + LANES, hidden), bf16),
            pltpu.VMEM((iters, rows, state_dim), f32),
            pltpu.VMEM((rows, state_dim), f32),
            pltpu.VMEM((iters, rows, LANES), f32),
            pltpu.VMEM((iters, cand_dev, env_dev, LANES), f32),
            pltpu.VMEM((units, SUB, LANES), f32),
            pltpu.VMEM((units, SUB, LANES), f32),
            pltpu.VMEM((iters, units, 2, SUB, LANES), f32),
            pltpu.VMEM((iters, n_cand - 1, share, 2, SUB, LANES), f32),
            pltpu.VMEM((iters, units, 2, SUB, LANES), f32),
            pltpu.VMEM((iters, 1, LANES), f32),
            pltpu.VMEM((iters, n_cand * n_env, 1, LANES), f32),
            pltpu.SemaphoreType.DMA((len(operands) + 1,)),
            pltpu.SemaphoreType.DMA((iters, 5)),
            pltpu.SemaphoreType.DMA((iters, 5)),
        ],
        compiler_params=pltpu.CompilerParams(collective_id=0, has_side_effects=True),
    )(*operands)
    fmean, fstd, cost = pl.pallas_call(
        store_kernel,
        out_shape=tuple(jax.ShapeDtypeStruct(shape, kind) for shape, kind in outs),
        in_specs=[vmem] * len(outs),
        out_specs=(hbm, hbm, hbm),
        scratch_shapes=[pltpu.SemaphoreType.DMA((len(outs),))],
    )(*(pltpu.with_memory_space_constraint(x, pltpu.VMEM) for x in (fmean, fstd, cost)))
    return fmean, fstd, jnp.swapaxes(cost, 1, 2)


def solution(mesh):
    in_specs = (
        P(None, "env", "cand", None),
        P("env", None),
        P("env", None),
        P("env", None),
        P("env", None),
        P(),
        P(),
        P(),
        P(),
        P(),
        P("env", None, None),
    )
    out_specs = (P("env", None), P("env", None), P(None, "env", "cand"))
    return jax.shard_map(shards, mesh=mesh, in_specs=in_specs, out_specs=out_specs, check_vma=False)
```
